512 devices in a mesh: learner: 32 (over x, y), tensor: 16 (over z, core).
Axes of the slice: x: 4, y: 8, z: 8, core: 2. Of those that a mesh axis runs over, the one named last changes fastest.
Arguments:
- blocks: bfloat16 [256, 128, 4096], P('learner', None, 'tensor'), may hold values from -60 to 60
- seg_ids: int32 [32, 1024], P('learner'), may hold values from 0 to 7, never falling along the last dimension, each value on 1 to 256 neighbouring positions
- dest: int32 [256], replicated, may hold values from 0 to 31, as said below
- slot: int32 [256], replicated, may hold values from 0 to 7, as said below
- norm_gain: bfloat16 [4096], P('tensor'), may hold values from 0.25 to 1.75
- w_query: bfloat16 [4096, 4096], P(None, 'tensor'), may hold values from -2 to 2
- w_keyval: bfloat16 [4096, 2048], P('learner'), may hold values from -2 to 2
Outputs:
- context: bfloat16 [32768, 4096], P('learner', 'tensor')
The draws below stay inside these ranges and needn't reach their ends.
Inputs may be any that keep to these rules, and one draw needn't show every extreme that they name: `dest`: each learner receives exactly 8 blocks; at most 1 of the blocks of one learner go to any one learner, and in every draw some learner sends exactly 1 block to one learner. `slot`: the blocks that one learner receives take the positions 0 to 7 of its packed row, one each.
All inputs are finite; a program needn't handle non-finite values.
Results may differ from the reference program's by a relative error of at most 0.012.
The reference program's roundings to bfloat16 on the way (of `packed`, `normed`, `queries`, `keyval` and `probs`) count: a program that leaves them out, or rounds other values in their place, can miss the bound.
Values may be sent and summed in bfloat16 or wider, within the bound.
No kernel may reach another device: no remote copies, remote signals or barrier semaphores. Data moves between devices by JAX's collectives and lax.ppermute only.
A program may use at most 64 MiB of HBM per device.

```python
import math
import jax
import jax.numpy as jnp
import numpy as np
from jax import lax

D = 4096
HEADS = 32
KV_HEADS = 8
HD = 128
BLOCK = 128
BLK_DEV = 8
PACK = 1024
TOKENS = 32768
N_LEARNER = 32


def routing_tables(key):
    base = jax.random.fold_in(key, 11)
    first_key, second_key, third_key = jax.random.split(base, 3)
    outer = jax.random.permutation(first_key, N_LEARNER).astype(jnp.int32)
    inner = jax.random.permutation(second_key, N_LEARNER).astype(jnp.int32)
    turns = jax.random.randint(third_key, (N_LEARNER,), 0, BLK_DEV).astype(jnp.int32)
    counter = jnp.arange(N_LEARNER * BLK_DEV, dtype=jnp.int32)
    source = counter // BLK_DEV
    within = counter % BLK_DEV
    targets = outer[(inner[source] + within) % N_LEARNER]
    places = (within + turns[targets]) % BLK_DEV
    return (targets.astype(jnp.int32), places.astype(jnp.int32))


def draw_dest(key, part):
    return routing_tables(key)[0]


def draw_slot(key, part):
    return routing_tables(key)[1]


def shared_weights(key):
    base = jax.random.fold_in(key, 7)
    query_key, keyval_key = jax.random.split(base, 2)
    w_query = jax.random.normal(query_key, (D, HEADS * HD), jnp.float32) / math.sqrt(D)
    w_keyval = jax.random.normal(keyval_key, (D, 2 * KV_HEADS * HD), jnp.float32) / math.sqrt(D)
    return (jnp.clip(w_query, -2.0, 2.0), jnp.clip(w_keyval, -2.0, 2.0))


def draw_w_query(key, part):
    return shared_weights(key)[0].astype(jnp.bfloat16)


def draw_w_keyval(key, part):
    return shared_weights(key)[1].astype(jnp.bfloat16)


def draw_blocks(key, part):
    base = jax.random.fold_in(key, 3)
    noise_key, scale_key = jax.random.split(base, 2)
    shape = (N_LEARNER * BLK_DEV, BLOCK, D)
    row_scale = jnp.exp(jax.random.uniform(scale_key, (N_LEARNER * BLK_DEV, BLOCK, 1), jnp.float32, 0.0, math.log(10.0)))
    values = jax.random.normal(noise_key, shape, jnp.float32) * row_scale
    return jnp.clip(values, -60.0, 60.0).astype(jnp.bfloat16)


def length_profile(count, total, limit, skew):
    weights = [(1 << 20) // math.isqrt(standing ** skew) + 1 for standing in range(2, count + 1)]
    spare, counts = total - limit - (count - 1), [1] * (count - 1)
    while spare > 0:
        movable = [i for i in range(count - 1) if counts[i] < limit]
        mass, left = sum([weights[i] for i in movable]), spare
        for i in movable:
            extra = min(limit - counts[i], max(1, left * weights[i] // mass), spare)
            counts[i] = counts[i] + extra
            spare = spare - extra
    return np.array([limit] + counts)


def ragged(rng, count, total, limit, lean):
    if count == 2:
        one = jax.random.randint(rng, (), max(1, total - limit), min(limit, total - 1) + 1)
        return jnp.stack([one, total - one])
    sizes = jnp.asarray(length_profile(count, total, limit, lean), jnp.int32)
    couples = (count - 1) // 2
    source_of, sink = sizes[1:1 + 2 * couples:2], sizes[2:2 + 2 * couples:2]
    room = jnp.minimum(source_of - 1, limit - sink)
    moved = jax.random.randint(jax.random.fold_in(rng, 1), (couples,), 0, 1 << 20) % (room + 1)
    sizes = sizes.at[1:1 + 2 * couples:2].set(source_of - moved).at[2:2 + 2 * couples:2].set(sink + moved)
    return sizes[jax.random.permutation(jax.random.fold_in(rng, 2), count)]


def setup_inputs(seed: int = 0) -> dict:
    key_list = jax.random.split(jax.random.key(seed), 8)
    blocks = draw_blocks(jax.random.fold_in(key_list[7], 71), 0)
    seg_ids = jax.vmap(lambda own: jnp.searchsorted(jnp.cumsum(ragged(own, 8, PACK, PACK // 4, 2)), jnp.arange(PACK), side="right"))(jax.random.split(key_list[1], N_LEARNER)).reshape((N_LEARNER, PACK)).astype(jnp.int32)
    dest = draw_dest(jax.random.fold_in(key_list[7], 71), 0)
    slot = draw_slot(jax.random.fold_in(key_list[7], 71), 0)
    norm_gain = jnp.clip(1.0 + 0.15 * jax.random.normal(key_list[4], (D,), jnp.float32), 0.25, 1.75).astype(jnp.bfloat16)
    w_query = draw_w_query(jax.random.fold_in(key_list[7], 71), 0)
    w_keyval = draw_w_keyval(jax.random.fold_in(key_list[7], 71), 0)
    return {"blocks": blocks, "seg_ids": seg_ids, "dest": dest, "slot": slot, "norm_gain": norm_gain, "w_query": w_query, "w_keyval": w_keyval}


def reference(blocks, seg_ids, dest, slot, norm_gain, w_query, w_keyval):
    positions = (dest * BLK_DEV + slot).astype(jnp.int32)
    packed = jnp.zeros_like(blocks).at[positions].set(blocks)
    packed = packed.reshape(N_LEARNER, BLK_DEV * BLOCK, D)
    group = HEADS // KV_HEADS

    def one_shard(shard_item):
        shard_rows, segment = shard_item
        widened = shard_rows.astype(jnp.float32)
        mean_sq = lax.optimization_barrier(jnp.mean(widened * widened, axis=-1, keepdims=True))
        normed = (widened * lax.rsqrt(mean_sq + 1e-05) * norm_gain.astype(jnp.float32)).astype(jnp.bfloat16)
        queries = jnp.dot(normed, w_query, preferred_element_type=jnp.float32).astype(jnp.bfloat16)
        keyval = jnp.dot(normed, w_keyval, preferred_element_type=jnp.float32).astype(jnp.bfloat16)
        length = shard_rows.shape[0]
        query_heads = queries.reshape(length, HEADS, HD).astype(jnp.float32)
        keyval_split = keyval.reshape(length, KV_HEADS, 2, HD).astype(jnp.float32)
        key_heads = jnp.repeat(keyval_split[:, :, 0], group, axis=1)
        value_heads = jnp.repeat(keyval_split[:, :, 1], group, axis=1)
        scores = jnp.einsum('qhd,khd->hqk', query_heads, key_heads) / math.sqrt(HD)
        index = jnp.arange(length, dtype=jnp.int32)
        allowed = (segment[:, None] == segment[None, :]) & (index[None, :] <= index[:, None])
        masked = jnp.where(allowed[None], scores, -1e+30)
        row_max = lax.optimization_barrier(jnp.max(masked, axis=-1, keepdims=True))
        exponent = jnp.where(allowed[None], jnp.exp(masked - row_max), 0.0)
        probs = (exponent / lax.optimization_barrier(jnp.sum(exponent, axis=-1, keepdims=True))).astype(jnp.bfloat16)
        context = jnp.einsum('hqk,khd->qhd', probs.astype(jnp.float32), value_heads)
        return context.astype(jnp.bfloat16).reshape(length, HEADS * HD)
    result = lax.map(one_shard, (packed, seg_ids))
    return result.reshape(TOKENS, HEADS * HD)
```

```python
import functools
import math

import jax
import jax.numpy as jnp
from jax import lax
from jax.experimental import pallas as pl
from jax.experimental.pallas import tpu as pltpu
from jax.sharding import Mesh
from jax.sharding import PartitionSpec as P

D = 4096
HEADS = 32
KV_HEADS = 8
HD = 128
BLOCK = 128
PACK = 1024
EPS = 1e-05
BF = jnp.bfloat16
F32 = jnp.float32

NX, NY, NZ, NC = 4, 8, 8, 2
XY = ("x", "y")
ZC = ("z", "c")
RING = [(z * 2 + c, ((z + (1 if c == 0 else -1)) % NZ) * 2 + c) for z in range(NZ) for c in range(NC)]
SWAP = [(t, t ^ 1) for t in range(NZ * NC)]

VMEM = pl.BlockSpec(memory_space=pltpu.VMEM)
SMEM = pl.BlockSpec(memory_space=pltpu.SMEM)
HALF = PACK // 2
GAIN_ROWS = 16


def call(body, out_shape, in_specs, name, flops=0, bytes_accessed=0, scratch=(), vmem=None):
    return pl.pallas_call(
        body,
        out_shape=out_shape,
        in_specs=in_specs,
        out_specs=jax.tree.map(lambda _: VMEM, out_shape),
        scratch_shapes=list(scratch),
        name=name,
        cost_estimate=pl.CostEstimate(flops=flops, bytes_accessed=bytes_accessed, transcendentals=0),
        compiler_params=pltpu.CompilerParams(vmem_limit_bytes=vmem),
    )


def cut_body(blocks_ref, out_ref):
    for b in range(8):
        for g in range(8):
            for lane in range(2):
                v = blocks_ref[b, 16 * g : 16 * g + 16, 128 * lane : 128 * lane + 128]
                out_ref[4 * g + lane, b] = v[:8]
                out_ref[4 * g + 2 + lane, b] = v[8:]


def sort_body(dest_ref, slot_ref, in_ref, a_ref, b_ref, buf):
    def step(i, _):
        for u in range(8):
            k = i * 8 + u
            s = slot_ref[k]
            buf[s // 4, dest_ref[k] * 4 + s % 4] = in_ref[k]
        return 0

    lax.fori_loop(0, 32, step, 0)
    a_ref[...] = buf[0]
    b_ref[...] = buf[1]


def join_body(in_ref, gain_ref, out_ref):
    for s in range(4):
        for g in range(8):
            for lane in range(2):
                v = jnp.concatenate([in_ref[4 * g + lane, s], in_ref[4 * g + 2 + lane, s]], axis=0)
                out_ref[128 * s + 16 * g : 128 * s + 16 * g + 16, 128 * lane : 128 * lane + 128] = v
    if out_ref.shape[0] > HALF:
        out_ref[HALF:, :] = jnp.broadcast_to(gain_ref[...], (GAIN_ROWS, 256))


def project(parts, table, w_refs, rows):
    scaled, squares = [], None
    for read_rows, read_gain, _ in parts:
        x = read_rows(rows).astype(F32)
        sq = x * x
        sq = sq[:, :128] + sq[:, 128:]
        squares = sq if squares is None else squares + sq
        scaled.append((x * read_gain().astype(F32)).astype(BF))
    sums = []
    for w_ref in w_refs:
        total = None
        for x, (_, _, slot) in zip(scaled, parts):
            w = w_ref[pl.ds(pl.multiple_of(table[slot] * 256, 256), 256), :]
            p = jnp.dot(x, w, preferred_element_type=F32)
            total = p if total is None else total + p
        sums.append(total)
    return sums, squares


def slice_of(a_ref, b_ref, index):
    def rows(r):
        ref, at = (a_ref, r) if r < HALF else (b_ref, r - HALF)
        if index is None:
            return ref[at : at + 256, :]
        return ref[index, at : at + 256, :]

    def gain():
        return a_ref[HALF : HALF + 1, :] if index is None else a_ref[index, HALF : HALF + 1, :]

    return rows, gain


def first_body(table, own_a, own_b, a1, b1, a2, b2, wq, wm, wr, wo, acc_ref):
    parts = [
        (*slice_of(own_a, own_b, None), 0),
        (*slice_of(a1, b1, 0), 1),
        (*slice_of(a1, b1, 1), 2),
        (*slice_of(a2, b2, 0), 3),
        (*slice_of(a2, b2, 1), 4),
    ]
    for r in range(0, PACK, 256):
        (q, m, v, o), sq = project(parts, table, (wq, wm, wr, wo), r)
        acc_ref[r : r + 256, 0:256] = q
        acc_ref[r : r + 256, 256:384] = m
        acc_ref[r : r + 256, 384:512] = v
        acc_ref[r : r + 256, 512:768] = o
        acc_ref[r : r + 256, 768:896] = sq


def second_body(table, acc_ref, a3, b3, a4, b4, wq, wm, wr, wo, own_ref, pay_ref):
    parts = [
        (*slice_of(a3, b3, 0), 5),
        (*slice_of(a3, b3, 1), 6),
        (*slice_of(a4, b4, None), 7),
    ]
    for r in range(0, PACK, 256):
        (q, m, v, o), sq = project(parts, table, (wq, wm, wr, wo), r)
        rows = slice(r, r + 256)
        own_ref[rows, 0:256] = q + acc_ref[rows, 0:256]
        m = m + acc_ref[rows, 256:384]
        v = v + acc_ref[rows, 384:512]
        own_ref[rows, 256:384] = m
        own_ref[rows, 384:512] = v
        pay_ref[rows, 0:256] = (o + acc_ref[rows, 512:768]).astype(BF)
        pay_ref[rows, 256:384] = v.astype(BF)
        pay_ref[rows, 384:512] = m.astype(BF)
        total = jnp.sum(sq + acc_ref[rows, 768:896], axis=-1, keepdims=True)
        total = jnp.broadcast_to(total, (256, 128))
        own_ref[rows, 512:640] = total
        high = total.astype(BF)
        low = (total - high.astype(F32)).astype(BF)
        lane = lax.broadcasted_iota(jnp.int32, (256, 128), 1)
        pay_ref[rows, 512:640] = jnp.where(lane < 64, high.astype(F32), low.astype(F32)).astype(BF)


def attend_body(core_ref, own_ref, got_ref, seg_row, seg_col, out_ref, q_s, k_s, v_s):
    is0 = core_ref[0] == 0
    for r in range(0, PACK, 256):
        rows = slice(r, r + 256)
        far = got_ref[rows, 512:640].astype(F32)
        total = own_ref[rows, 512:513] + far[:, 0:1] + far[:, 64:65]
        inverse = lax.rsqrt(total * (1.0 / D) + EPS)
        both = (own_ref[rows, 0:512] + got_ref[rows, 0:512].astype(F32)) * inverse
        q_s[rows, :] = both[:, 0:256].astype(BF)
        mine, theirs = both[:, 256:384], both[:, 384:512]
        k_s[rows, :] = jnp.where(is0, mine, theirs).astype(BF)
        v_s[rows, :] = jnp.where(is0, theirs, mine).astype(BF)
    for i in range(8):
        low = max(0, i - 2) * 128
        high = (i + 1) * 128
        width = high - low
        rows = slice(i * 128, i * 128 + 128)
        k = k_s[low:high, :]
        v = v_s[low:high, :]
        q_at = lax.broadcasted_iota(jnp.int32, (128, width), 0) + (i * 128 - low)
        k_at = lax.broadcasted_iota(jnp.int32, (128, width), 1)
        allowed = (seg_col[rows, :] == seg_row[:, low:high]) & (k_at <= q_at)
        for h in range(2):
            q = q_s[rows, h * 128 : h * 128 + 128]
            s = lax.dot_general(q, k, (((1,), (1,)), ((), ())), preferred_element_type=F32)
            s = jnp.where(allowed, s * (1.0 / math.sqrt(HD)), -1e30)
            e = jnp.exp(s - jnp.max(s, axis=-1, keepdims=True))
            e = jnp.where(allowed, e, 0.0)
            p = (e / jnp.sum(e, axis=-1, keepdims=True)).astype(BF)
            o = jnp.dot(p, v, preferred_element_type=F32)
            out_ref[rows, h * 128 : h * 128 + 128] = o.astype(BF)


def shape(dims, dtype=BF):
    return jax.ShapeDtypeStruct(dims, dtype)


def to_all(x, axis):
    count = lax.axis_size(axis)
    return lax.all_to_all(jnp.broadcast_to(x[None], (count, *x.shape)), axis, 0, 0, tiled=True)


def on_device(blocks, seg_ids, dest, slot, norm_gain, w_query, w_keyval):
    z = lax.axis_index("z")
    core = lax.axis_index("c")
    pieces = call(cut_body, shape((32, 8, 8, 128)), [VMEM], "cut", bytes_accessed=1 << 20)(blocks)
    spread = lax.all_to_all(pieces, XY, 0, 0, tiled=True).reshape(256, 8, 128)
    low, high = call(
        sort_body,
        (shape((128, 8, 128)), shape((128, 8, 128))),
        [SMEM, SMEM, VMEM],
        "sort",
        flops=1 << 20,
        bytes_accessed=1 << 20,
        scratch=[pltpu.VMEM((2, 128, 8, 128), BF)],
    )(dest, slot, spread)
    gain = norm_gain.reshape(1, 256)
    halves = []
    for part, rows in ((low, HALF + GAIN_ROWS), (high, HALF)):
        came = lax.all_to_all(part.reshape(32, 4, 8, 128), XY, 0, 0, tiled=True)
        halves.append(
            call(join_body, shape((rows, 256)), [VMEM, VMEM], "join", bytes_accessed=1 << 19)(came, gain)
        )
    own_a, own_b = halves

    wq_other = lax.ppermute(w_query, ZC, SWAP)
    kv_cols = lax.dynamic_slice_in_dim(w_keyval, (2 * z + core) * HD, HD, 1)
    kv_rows = to_all(to_all(kv_cols, "y"), "x").reshape(D, HD)
    kv_other = lax.ppermute(kv_rows, ZC, SWAP)

    a = jnp.stack([own_a, lax.ppermute(own_a, ZC, SWAP)])
    b = jnp.stack([own_b, lax.ppermute(own_b, ZC, SWAP)])
    got = []
    for _ in range(3):
        a = lax.ppermute(a, ZC, RING)
        b = lax.ppermute(b, ZC, RING)
        got.append((a, b))
    a4 = lax.ppermute(a[0], ZC, RING)
    b4 = lax.ppermute(b[0], ZC, RING)
    (a1, b1), (a2, b2), (a3, b3) = got

    turn = 2 * core - 1
    chips = [(z + turn * k) % NZ for k in range(5)]
    order = [2 * chips[0] + core]
    for k in (1, 2, 3):
        order += [2 * chips[k] + core, 2 * chips[k] + 1 - core]
    order.append(2 * chips[4] + core)
    table = jnp.stack(order).astype(jnp.int32)

    weights = (w_query, kv_rows, kv_other, wq_other)
    acc = call(
        first_body,
        shape((PACK, 896), F32),
        [SMEM] + [VMEM] * 10,
        "first",
        flops=2 * PACK * 1280 * 768,
        bytes_accessed=12 << 20,
    )(table, own_a, own_b, a1, b1, a2, b2, *weights)
    own, pay = call(
        second_body,
        (shape((PACK, 640), F32), shape((PACK, 640))),
        [SMEM] + [VMEM] * 9,
        "second",
        flops=2 * PACK * 768 * 768,
        bytes_accessed=12 << 20,
    )(table, acc, a3, b3, a4, b4, *weights)
    far = lax.ppermute(pay, ZC, SWAP)
    return call(
        attend_body,
        shape((PACK, 256)),
        [SMEM] + [VMEM] * 4,
        "attend",
        flops=4 * PACK * 384 * 256,
        bytes_accessed=5 << 20,
        scratch=[pltpu.VMEM((PACK, 256), BF), pltpu.VMEM((PACK, 128), BF), pltpu.VMEM((PACK, 128), BF)],
    )(core.reshape(1), own, far, seg_ids, seg_ids.reshape(PACK, 1))


def solution(mesh):
    fine = Mesh(mesh.devices.reshape(NX, NY, NZ, NC), ("x", "y", "z", "c"))
    return jax.shard_map(
        on_device,
        mesh=fine,
        in_specs=(P(XY, None, ZC), P(XY, None), P(), P(), P(ZC), P(None, ZC), P(XY, None)),
        out_specs=P(XY, ZC),
        check_vma=False,
    )
```
